32 devices in a mesh: fsdp: 2 (over y), trow: 4 (over x, core), tcol: 4 (over z).
Axes of the slice: x: 2, y: 2, z: 4, core: 2. Of those that a mesh axis runs over, the one named last changes fastest.
Arguments:
- tokens: bfloat16 [512, 4096], P('fsdp', 'tcol'), may hold values from -100 to 100
- w_up: bfloat16 [4096, 16384], P('tcol', ('fsdp', 'trow')), may hold values from -0.1875 to 0.1875
- w_down: bfloat16 [16384, 4096], P(('fsdp', 'trow'), 'tcol'), may hold values from -0.046875 to 0.046875
- cotangent: bfloat16 [512, 4096], P('fsdp', 'tcol'), may hold values from -6 to 6
Outputs:
- mixed: bfloat16 [512, 4096], P('fsdp', 'tcol')
- input_gradient: bfloat16 [512, 4096], P('fsdp', 'tcol')
- grad_up: bfloat16 [4096, 16384], P('tcol', ('fsdp', 'trow'))
- grad_down: bfloat16 [16384, 4096], P(('fsdp', 'trow'), 'tcol')
The draws below stay inside these ranges and needn't reach their ends.
All inputs are finite; a program needn't handle non-finite values.
Results may differ from the reference program's by a relative error of at most 0.02.
Values may be sent and summed in bfloat16 or wider, within the bound.
No kernel may reach another device: no remote copies, remote signals or barrier semaphores. Data moves between devices by JAX's collectives and lax.ppermute only.
A program may use at most 128 MiB of HBM per device.

```python
import jax
import jax.numpy as jnp
from jax import lax

MODEL_WIDTH = 4096
FF = 16384
TOK_GRP = 256
TOKENS = 512
N_FSDP = 2
N_TCOL = 4


def draw_tokens(key, part):
    keys = jax.random.split(jax.random.fold_in(key, 17), 3)
    rising = jnp.exp(jnp.log(3.0) * jnp.arange(MODEL_WIDTH, dtype=jnp.float32) / (MODEL_WIDTH - 1))
    column = rising * jnp.exp(jax.random.uniform(keys[1], (MODEL_WIDTH,), jnp.float32, 0.0, jnp.log(10.0))) / jnp.sqrt(30.0)
    base = jnp.clip(jax.random.normal(keys[0], (TOKENS, MODEL_WIDTH), jnp.float32), -4.0, 4.0)
    row = jnp.exp(jax.random.uniform(keys[2], (TOKENS, 1), jnp.float32, 0.0, jnp.log(10.0))) / jnp.sqrt(10.0)
    return (base * row * column[None, :]).astype(jnp.bfloat16)


def draw_w_up(key, part):
    keys = jax.random.split(jax.random.fold_in(key, 29), 2)
    position = jnp.arange(MODEL_WIDTH, dtype=jnp.float32) / (MODEL_WIDTH - 1)
    shared = jnp.clip(jax.random.normal(keys[1], (1, FF), jnp.float32), -3.0, 3.0)
    rising = jnp.exp(jnp.log(4.0) * position)
    noise = jnp.clip(jax.random.normal(keys[0], (MODEL_WIDTH, FF), jnp.float32), -4.0, 4.0)
    strength = 0.5
    rising = rising / jnp.sqrt(jnp.mean(rising * rising))
    values = rising[:, None] * (noise + strength * shared) / jnp.sqrt(1.0 * MODEL_WIDTH)
    return values.astype(jnp.bfloat16)


def shard_levels(own_key, dims, cuts, low, high):
    def one(dim, parts):
        steps = jax.random.uniform(jax.random.fold_in(jax.random.fold_in(own_key, 6), dim), (parts,), jnp.float32, low / len(cuts), high / len(cuts))
        return jnp.repeat(jnp.exp(steps), dims[dim] // parts).reshape((-1,) + (1,) * (len(dims) - dim - 1))

    level = one(*cuts[0])
    for cut in cuts[1:]:
        level = level * one(*cut)
    return level


def bell_draw(stream_key, shape, spread, reach, shards=(), kind=jnp.bfloat16):
    result = spread * jax.random.normal(stream_key, shape, jnp.float32)
    if shards:
        result = result * shard_levels(stream_key, shape, shards, -0.22, 0.18)
    return jnp.clip(result, -reach, reach).astype(kind)


def setup_inputs(seed: int = 0) -> dict:
    key_of = jax.random.split(jax.random.key(seed), 5)
    return {
        "tokens": draw_tokens(jax.random.fold_in(key_of[4], 71), 0),
        "w_up": draw_w_up(jax.random.fold_in(key_of[4], 71), 0),
        "w_down": bell_draw(key_of[2], (FF, MODEL_WIDTH), FF ** -0.5, 0.046875, ((0, 8), (1, 4))),
        "cotangent": bell_draw(key_of[3], (TOKENS, MODEL_WIDTH), 1.0, 6.0, ((0, 2), (1, 4))),
    }


def gelu_value(pre):
    phi = 0.5 * (1.0 + jax.scipy.special.erf(pre * 0.7071067811865476))
    return pre * phi

def gelu_slope(pre):
    phi = 0.5 * (1.0 + jax.scipy.special.erf(pre * 0.7071067811865476))
    return phi + pre * jnp.exp(-0.5 * pre * pre) * 0.3989422804014327

def rounded_term(value):
    low = lax.optimization_barrier(value.astype(jnp.bfloat16))
    return low.astype(jnp.float32)

def reference(tokens, w_up, w_down, cotangent):
    block = MODEL_WIDTH // N_TCOL
    input_float = tokens.astype(jnp.float32)
    token_mean = lax.optimization_barrier(jnp.sum(input_float, axis=1)) / MODEL_WIDTH
    var = lax.optimization_barrier(jnp.sum(input_float * input_float, axis=1)) / MODEL_WIDTH - token_mean * token_mean
    inverse_stddev = lax.rsqrt(var + 1e-05)
    centered_scaled = (input_float - token_mean[:, None]) * inverse_stddev[:, None]
    normalized_rows = centered_scaled.astype(jnp.bfloat16)

    def pre_step(index, total):
        start = (index * block).astype(jnp.int32)
        left = lax.dynamic_slice_in_dim(normalized_rows, start, block, 1)
        right = lax.dynamic_slice_in_dim(w_up, start, block, 0)
        return total + rounded_term(jnp.dot(left, right, preferred_element_type=jnp.float32))
    pre = lax.fori_loop(0, N_TCOL, pre_step, jnp.zeros((TOKENS, FF), jnp.float32))
    hidden = gelu_value(pre).astype(jnp.bfloat16)
    branch = jnp.dot(hidden, w_down, preferred_element_type=jnp.float32)
    mixed = (input_float + branch).astype(jnp.bfloat16)

    def down_step(index, total):
        start = (index * TOK_GRP).astype(jnp.int32)
        left = lax.dynamic_slice_in_dim(hidden, start, TOK_GRP, 0)
        right = lax.dynamic_slice_in_dim(cotangent, start, TOK_GRP, 0)
        part = lax.dot_general(left, right, (((0,), (0,)), ((), ())), preferred_element_type=jnp.float32)
        return total + rounded_term(part)
    grad_down = lax.fori_loop(0, N_FSDP, down_step, jnp.zeros((FF, MODEL_WIDTH), jnp.float32))

    def dh_step(index, total):
        start = (index * block).astype(jnp.int32)
        left = lax.dynamic_slice_in_dim(cotangent, start, block, 1)
        right = lax.dynamic_slice_in_dim(w_down, start, block, 1)
        part = lax.dot_general(left, right, (((1,), (1,)), ((), ())), preferred_element_type=jnp.float32)
        return total + rounded_term(part)
    dhid = lax.fori_loop(0, N_TCOL, dh_step, jnp.zeros((TOKENS, FF), jnp.float32))
    dpre = (dhid * gelu_slope(pre)).astype(jnp.bfloat16)

    def up_step(index, total):
        start = (index * TOK_GRP).astype(jnp.int32)
        left = lax.dynamic_slice_in_dim(normalized_rows, start, TOK_GRP, 0)
        right = lax.dynamic_slice_in_dim(dpre, start, TOK_GRP, 0)
        part = lax.dot_general(left, right, (((0,), (0,)), ((), ())), preferred_element_type=jnp.float32)
        return total + rounded_term(part)
    grad_up = lax.fori_loop(0, N_FSDP, up_step, jnp.zeros((MODEL_WIDTH, FF), jnp.float32))
    normed_gradient = lax.dot_general(dpre, w_up, (((1,), (1,)), ((), ())), preferred_element_type=jnp.float32)
    first_moment = lax.optimization_barrier(jnp.sum(normed_gradient, axis=1)) / MODEL_WIDTH
    second_moment = lax.optimization_barrier(jnp.sum(normed_gradient * centered_scaled, axis=1)) / MODEL_WIDTH
    input_gradient = cotangent.astype(jnp.float32) + inverse_stddev[:, None] * (normed_gradient - first_moment[:, None] - centered_scaled * second_moment[:, None])
    return (mixed, input_gradient.astype(jnp.bfloat16), grad_up.astype(jnp.bfloat16), grad_down.astype(jnp.bfloat16))
```

```python
import jax
import jax.numpy as jnp
from jax import lax
from jax.sharding import PartitionSpec as P


def gelu_value(pre):
    phi = 0.5 * (1.0 + jax.scipy.special.erf(pre * 0.7071067811865476))
    return pre * phi


def gelu_slope(pre):
    phi = 0.5 * (1.0 + jax.scipy.special.erf(pre * 0.7071067811865476))
    return phi + pre * jnp.exp(-0.5 * pre * pre) * 0.3989422804014327


def contract(left, right, left_dim, right_dim):
    return lax.dot_general(
        left, right, (((left_dim,), (right_dim,)), ((), ())), preferred_element_type=jnp.float32
    )


def local(tokens, w_up, w_down, cotangent):
    width = tokens.shape[1] * lax.axis_size("tcol")
    input_float = tokens.astype(jnp.float32)
    cot_all = lax.all_gather(cotangent, "fsdp", axis=0, tiled=True)
    sum_one, sum_two = lax.psum(
        (jnp.sum(input_float, axis=1), jnp.sum(input_float * input_float, axis=1)), "tcol"
    )
    token_mean = sum_one / width
    var = sum_two / width - token_mean * token_mean
    inverse_stddev = lax.rsqrt(var + 1e-05)
    centered_scaled = (input_float - token_mean[:, None]) * inverse_stddev[:, None]
    normed = lax.all_gather(centered_scaled.astype(jnp.bfloat16), "fsdp", axis=0, tiled=True)
    dhid = lax.psum(contract(cot_all, w_down, 1, 1).astype(jnp.bfloat16), "tcol").astype(jnp.float32)
    pre = lax.psum(contract(normed, w_up, 1, 0).astype(jnp.bfloat16), "tcol").astype(jnp.float32)
    hidden = gelu_value(pre).astype(jnp.bfloat16)
    dpre = (dhid * gelu_slope(pre)).astype(jnp.bfloat16)
    branch = lax.psum_scatter(
        contract(hidden, w_down, 1, 0).astype(jnp.bfloat16), "fsdp", scatter_dimension=0, tiled=True
    )
    branch = lax.psum(branch, "trow").astype(jnp.float32)
    mixed = (input_float + branch).astype(jnp.bfloat16)
    dnorm = lax.psum_scatter(
        contract(dpre, w_up, 1, 1).astype(jnp.bfloat16), "fsdp", scatter_dimension=0, tiled=True
    )
    dnorm = lax.psum(dnorm, "trow").astype(jnp.float32)
    grad_down = contract(hidden, cot_all, 0, 0).astype(jnp.bfloat16)
    grad_up = contract(normed, dpre, 0, 0).astype(jnp.bfloat16)
    mean_first, mean_second = lax.psum(
        (jnp.sum(dnorm, axis=1), jnp.sum(dnorm * centered_scaled, axis=1)), "tcol"
    )
    first_moment = mean_first / width
    second_moment = mean_second / width
    input_gradient = cotangent.astype(jnp.float32) + inverse_stddev[:, None] * (
        dnorm - first_moment[:, None] - centered_scaled * second_moment[:, None]
    )
    return (mixed, input_gradient.astype(jnp.bfloat16), grad_up, grad_down)


def solution(mesh):
    return jax.shard_map(
        local,
        mesh=mesh,
        in_specs=(
            P("fsdp", "tcol"),
            P("tcol", ("fsdp", "trow")),
            P(("fsdp", "trow"), "tcol"),
            P("fsdp", "tcol"),
        ),
        out_specs=(
            P("fsdp", "tcol"),
            P("fsdp", "tcol"),
            P("tcol", ("fsdp", "trow")),
            P(("fsdp", "trow"), "tcol"),
        ),
        check_vma=False,
    )
```
